256 devices in a mesh: py: 4 (over x), px: 4 (over y), pz: 16 (over z, core).
Axes of the slice: x: 4, y: 4, z: 8, core: 2. Of those that a mesh axis runs over, the one named last changes fastest.
Arguments:
- tracer: float32 [32, 384, 128, 128], P('py', 'px', 'pz'), may hold values from 0.2 to 1.8
- flow_y: float32 [32, 384, 128, 128], P('py', 'px', 'pz'), may hold values from -0.3 to 0.3
- flow_x: float32 [32, 384, 128, 128], P('py', 'px', 'pz'), may hold values from -0.3 to 0.3
- flow_z: float32 [32, 384, 128, 128], P('py', 'px', 'pz'), may hold values from -0.3 to 0.3
Outputs:
- potential: float32 [32, 384, 128, 128], P('py', 'px', 'pz')
- tracer_end: float32 [32, 384, 128, 128], P('py', 'px', 'pz')
The draws below stay inside these ranges and needn't reach their ends.
All inputs are finite; a program needn't handle non-finite values.
Results may differ from the reference program's by a relative error of at most 0.00002.
Values sent between devices are 32-bit elements; how exact they have to be, the bound alone decides.
No kernel may reach another device: no remote copies, remote signals or barrier semaphores. Data moves between devices by JAX's collectives and lax.ppermute only.
A program may use at most 128 MiB of HBM per device.

```python
import jax
import jax.numpy as jnp
from jax import lax

GRID_Y = 32
GRID_X = 384
GRID_Z = 128
MEMBERS = 128
STEPS = 4


def shard_levels(stream_key, shape, cuts, smallest, largest):
    def one(dim, parts):
        steps = jax.random.uniform(jax.random.fold_in(jax.random.fold_in(stream_key, 6), dim), (parts,), jnp.float32, smallest / len(cuts), largest / len(cuts))
        return jnp.repeat(jnp.exp(steps), shape[dim] // parts).reshape((-1,) + (1,) * (len(shape) - dim - 1))

    gain = one(*cuts[0])
    for cut in cuts[1:]:
        gain = gain * one(*cut)
    return gain


def setup_inputs(seed: int = 0) -> dict:
    streams_of = jax.random.split(jax.random.key(seed), 5)
    return {
        "tracer": jnp.clip(0.2 + 1.5999999 * jax.random.uniform(streams_of[0], (GRID_Y, GRID_X, GRID_Z, MEMBERS), jnp.float32) ** shard_levels(streams_of[0], (GRID_Y, GRID_X, GRID_Z, MEMBERS), ((0, 4), (1, 4), (2, 16)), -0.2, 0.2), 0.2, 1.8),
        "flow_y": jnp.clip(jax.random.uniform(streams_of[1], (GRID_Y, GRID_X, GRID_Z, MEMBERS), jnp.float32, -0.3, 0.3) * shard_levels(streams_of[1], (GRID_Y, GRID_X, GRID_Z, MEMBERS), ((0, 4), (1, 4), (2, 16)), -0.4, 0.0), -0.3, 0.3),
        "flow_x": jnp.clip(jax.random.uniform(streams_of[2], (GRID_Y, GRID_X, GRID_Z, MEMBERS), jnp.float32, -0.3, 0.3) * shard_levels(streams_of[2], (GRID_Y, GRID_X, GRID_Z, MEMBERS), ((0, 4), (1, 4), (2, 16)), -0.4, 0.0), -0.3, 0.3),
        "flow_z": jnp.clip(jax.random.uniform(streams_of[3], (GRID_Y, GRID_X, GRID_Z, MEMBERS), jnp.float32, -0.3, 0.3) * shard_levels(streams_of[3], (GRID_Y, GRID_X, GRID_Z, MEMBERS), ((0, 4), (1, 4), (2, 16)), -0.4, 0.0), -0.3, 0.3),
    }


def strip_edges(values, dims):
    for dim in dims:
        values = lax.slice_in_dim(values, 1, values.shape[dim] - 1, axis=dim)
    return values


def neighbour(values, dim, start, dims):
    others = [other for other in dims if other != dim]
    values = strip_edges(values, others)
    return lax.slice_in_dim(values, start, start + values.shape[dim] - 2, axis=dim)


def one_step(padded, flow_y, flow_x, flow_z):
    middle = strip_edges(padded, (0, 1, 2))
    lower = [neighbour(padded, dim, 0, (0, 1, 2)) for dim in (0, 1, 2)]
    upper = [neighbour(padded, dim, 2, (0, 1, 2)) for dim in (0, 1, 2)]
    slopes = [above - below for above, below in zip(upper, lower)]
    smooth_rate = 0.05
    spread = lower[0] + upper[0] + lower[1] + upper[1] + lower[2] + upper[2] - 6.0 * middle
    return middle - flow_y * slopes[0] - flow_x * slopes[1] - flow_z * slopes[2] + smooth_rate * spread


def reference(tracer, flow_y, flow_x, flow_z):
    for step in range(STEPS):
        tracer = one_step(jnp.pad(tracer, ((1, 1), (1, 1), (1, 1), (0, 0)), mode="constant"), flow_y, flow_x, flow_z)
    potential = jnp.cumsum(tracer, axis=2) / GRID_Z
    return potential, tracer
```

```python
import functools

import jax
import jax.numpy as jnp
from jax import lax
from jax.experimental import pallas as pl
from jax.experimental.pallas import tpu as pltpu
from jax.sharding import PartitionSpec as P

STEPS = 4
RATE = 0.05
VMEM = pltpu.VMEM
SMEM = pltpu.SMEM
LIMIT = 8 * 1024 * 1024


def pairs(n, k):
    perm = []
    for i in range(k, n, 2):
        j = (i + 1) % n
        perm += [(i, j), (j, i)]
    return perm


def flip(n, bit):
    return [(i, i ^ bit) for i in range(n)]


def call(body, outs, args, flops=1_000_000, aliases=None, scratch=()):
    table, *rest = args
    in_specs, operands = [pl.BlockSpec(memory_space=SMEM)], [table]
    for a in rest:
        if isinstance(a, tuple):
            in_specs.append(pl.BlockSpec(memory_space=pltpu.HBM))
            operands.append(pltpu.with_memory_space_constraint(a[0], pltpu.HBM))
        else:
            in_specs.append(pl.BlockSpec(memory_space=VMEM))
            operands.append(pltpu.with_memory_space_constraint(a, VMEM))
    outs = outs if isinstance(outs, tuple) else (outs,)
    out_specs = [
        pl.BlockSpec(memory_space=pltpu.HBM if isinstance(o, jax.ShapeDtypeStruct) else VMEM)
        for o in outs
    ]
    result = pl.pallas_call(
        body,
        out_shape=outs,
        in_specs=in_specs,
        out_specs=tuple(out_specs),
        scratch_shapes=scratch,
        input_output_aliases=aliases or {},
        compiler_params=pltpu.CompilerParams(vmem_limit_bytes=LIMIT),
        cost_estimate=pl.CostEstimate(flops=flops, bytes_accessed=1024, transcendentals=0),
    )(*operands)
    return result if len(outs) > 1 else result[0]


ODD_Y, ODD_X, ODD_Z, IN_Y, IN_X, IN_Z, BIT_1, BIT_2, BIT_3 = range(9)


def table():
    rows = []
    for name in ("py", "px", "pz"):
        i = lax.axis_index(name)
        rows.append(i % 2)
    for name in ("py", "px", "pz"):
        i = lax.axis_index(name)
        n = lax.axis_size(name)
        rows.append(jnp.where((i == 0) | (i == n - 1), 0, 1))
    rows += [(lax.axis_index("pz") // k) % 2 for k in (2, 4, 8)]
    return jnp.stack(rows).astype(jnp.int32)


def y_faces(s, t, ya, yb):
    ny, nx, _, _ = t.shape
    odd = s[ODD_Y] == 1
    keep = s[IN_Y].astype(jnp.float32)

    def rows(i, _):
        lo, hi = t[0, i], t[ny - 1, i]
        ya[i] = jnp.where(odd, lo, hi)
        yb[i] = jnp.where(odd, hi, lo) * keep
        return 0

    lax.fori_loop(0, nx, rows, 0, unroll=8)


def first_kernel(s, t, ya, yb, sem):
    ny = t.shape[0]
    odd = s[ODD_Y]
    copies = [
        pltpu.make_async_copy(t.at[(ny - 1) * (1 - odd)], ya, sem.at[0]),
        pltpu.make_async_copy(t.at[(ny - 1) * odd], yb, sem.at[1]),
    ]
    for c in copies:
        c.start()
    for c in copies:
        c.wait()
    keep = s[IN_Y].astype(jnp.float32)

    def rows(i, _):
        yb[i] = yb[i] * keep
        return 0

    lax.fori_loop(0, ya.shape[0], rows, 0, unroll=8)


def face_kernel(s, t, za, zb, xa, xb):
    ny, nx, nz, _ = t.shape
    odd_z = s[ODD_Z] == 1
    keep_z = s[IN_Z].astype(jnp.float32)
    flat = t.reshape(ny * nx * nz, 128)
    za_f, zb_f = za.reshape(ny * nx, 128), zb.reshape(ny * nx, 128)

    def cols(i, _):
        base = pl.multiple_of(i * 8 * nz, 8 * nz)
        lo = flat[pl.ds(base, 8, stride=nz), :]
        hi = flat[pl.ds(base + nz - 1, 8, stride=nz), :]
        at = pl.ds(pl.multiple_of(i * 8, 8), 8)
        za_f[at, :] = jnp.where(odd_z, lo, hi)
        zb_f[at, :] = jnp.where(odd_z, hi, lo) * keep_z
        return 0

    lax.fori_loop(0, ny * nx // 8, cols, 0, unroll=8)
    odd_x = s[ODD_X] == 1
    keep_x = s[IN_X].astype(jnp.float32)
    for y in range(ny):
        lo, hi = t[y, 0], t[y, nx - 1]
        xa[y] = jnp.where(odd_x, lo, hi)
        xb[y] = jnp.where(odd_x, hi, lo) * keep_x


def main_kernel(s, t, fy, fx, fz, za, zb, xa, xb, out, zl, zh):
    ny, nx, nz, _ = t.shape
    odd_z = s[ODD_Z] == 1
    odd_x = s[ODD_X] == 1
    za_f, zb_f = za.reshape(ny * nx, 128), zb.reshape(ny * nx, 128)

    def order(i, _):
        at = pl.ds(pl.multiple_of(i * 8, 8), 8)
        a, b = za_f[at, :], zb_f[at, :]
        zl[at, :] = jnp.where(odd_z, a, b)
        zh[at, :] = jnp.where(odd_z, b, a)
        return 0

    lax.fori_loop(0, ny * nx // 8, order, 0, unroll=8)
    iota = lax.broadcasted_iota(jnp.int32, (nz, 128), 0)
    is_lo, is_hi = iota == 0, iota == nz - 1

    def cell(y, x, back, mid, ahead, down_y, up_y):
        row = y * nx + x
        lo = jnp.broadcast_to(zl[pl.ds(row, 1), :], (nz, 128))
        hi = jnp.broadcast_to(zh[pl.ds(row, 1), :], (nz, 128))
        down_z = jnp.where(is_lo, lo, pltpu.roll(mid, 1, axis=0))
        up_z = jnp.where(is_hi, hi, pltpu.roll(mid, nz - 1, axis=0))
        spread = (down_z + up_z) + (back + ahead)
        slope = fx[y, x] * (ahead - back) + fz[y, x] * (up_z - down_z)
        if down_y is None:
            slope = slope + fy[y, x] * up_y
            spread = spread + up_y
        elif up_y is None:
            slope = slope - fy[y, x] * down_y
            spread = spread + down_y
        else:
            slope = slope + fy[y, x] * (up_y - down_y)
            spread = spread + (up_y + down_y)
        out[y, x] = (1.0 - 6.0 * RATE) * mid - slope + RATE * spread

    def line(y, first, last):
        a, b = xa[y], xb[y]
        x_lo = jnp.where(odd_x, a, b)
        x_hi = jnp.where(odd_x, b, a)

        def step(x, back, mid, ahead):
            cell(
                y, x, back, mid, ahead,
                None if first else t[y - 1, x],
                None if last else t[y + 1, x],
            )

        def body(x, carry):
            back, mid = carry
            ahead = t[y, x + 1]
            step(x, back, mid, ahead)
            return mid, ahead

        back, mid = lax.fori_loop(0, nx - 1, body, (x_lo, t[y, 0]), unroll=5)
        step(nx - 1, back, mid, x_hi)

    line(0, True, False)
    lax.fori_loop(1, ny - 1, lambda y, _: (line(y, False, False), 0)[1], 0)
    line(ny - 1, False, True)


def fix_rows(s, u, fy, ya, yb):
    ny, nx, _, _ = u.shape
    odd = s[ODD_Y] == 1

    def body(x, _):
        a, b = ya[x], yb[x]
        lo, hi = jnp.where(odd, a, b), jnp.where(odd, b, a)
        u[0, x] = u[0, x] + (RATE + fy[0, x]) * lo
        u[ny - 1, x] = u[ny - 1, x] + (RATE - fy[ny - 1, x]) * hi
        return 0

    lax.fori_loop(0, nx, body, 0, unroll=8)


def fix_kernel(s, u_in, fy, ya_in, yb_in, u, ya, yb):
    del u_in
    fix_rows(s, u, fy, ya_in, yb_in)
    y_faces(s, u, ya, yb)


def last_kernel(s, u_in, fy, ya_in, yb_in, u, out, run, mine, other, sem):
    del u_in
    ny, nx, nz, _ = u.shape
    fix_rows(s, u, fy, ya_in, yb_in)
    copies = [pltpu.make_async_copy(u.at[y], out.at[y], sem.at[y]) for y in range(ny)]
    for c in copies:
        c.start()
    iota = lax.broadcasted_iota(jnp.int32, (nz, 128), 0)
    keep = [iota >= d for d in (1, 2, 4)]

    def line(y, _):
        def body(x, _):
            v = u[y, x]
            for d, m in zip((1, 2, 4), keep):
                v = v + jnp.where(m, pltpu.roll(v, d, axis=0), 0.0)
            run[y, x] = v
            return 0

        return lax.fori_loop(0, nx, body, 0, unroll=8)

    lax.fori_loop(0, ny, line, 0)
    flat = run.reshape(ny * nx * nz, 128)
    half = ny * nx // 2
    mine_f, other_f = mine.reshape(half, 128), other.reshape(half, 128)
    odd = s[ODD_Z]

    def cols(i, _):
        at = pl.ds(pl.multiple_of(i * 8, 8), 8)
        for bit, ref in ((odd, mine_f), (1 - odd, other_f)):
            base = pl.multiple_of((bit * half + i * 8) * nz, 8 * nz)
            ref[at, :] = flat[pl.ds(base + nz - 1, 8, stride=nz), :]
        return 0

    lax.fori_loop(0, half // 8, cols, 0, unroll=8)
    for c in copies:
        c.wait()


def over_rows(ref, body, unroll=8):
    def step(i, _):
        body(pl.ds(pl.multiple_of(i * 8, 8), 8))
        return 0

    lax.fori_loop(0, ref.shape[0] // 8, step, 0, unroll=unroll)


def halve_kernel(s, mine, r, mine2, other2):
    half = mine2.shape[0]
    bit = s[BIT_1]

    def body(at):
        for b, ref in ((bit, mine2), (1 - bit, other2)):
            src = pl.ds(pl.multiple_of(b * half + at.start, 8), 8)
            ref[at, :] = mine[src, :] + r[src, :]

    over_rows(mine2, body)


def add_kernel(s, a, b, out):
    del s

    def body(at):
        out[at, :] = a[at, :] + b[at, :]

    over_rows(out, body)


def back_kernel(s, mine2, r2, q, q2, sent, kept):
    b1, b2, b3 = (s[k].astype(jnp.float32) for k in (BIT_1, BIT_2, BIT_3))

    def body(at):
        pre = b2 * q[at, :] + b3 * q2[at, :]
        sent[at, :] = pre + (1.0 - b1) * mine2[at, :]
        kept[at, :] = pre + b1 * r2[at, :]

    over_rows(sent, body)


def core_kernel(s, mine, r, kept1, got1, sent, kept):
    half = kept1.shape[0]
    odd = s[ODD_Z].astype(jnp.float32)
    bit = s[BIT_1]

    def body(at):
        for b, ref in ((bit, kept1), (1 - bit, got1)):
            dst = pl.ds(pl.multiple_of(b * half + at.start, 8), 8)
            pre = ref[at, :]
            sent[dst, :] = pre + (1.0 - odd) * mine[dst, :]
            kept[dst, :] = pre + odd * r[dst, :]

    over_rows(kept1, body)


def end_kernel(s, run, own, got, out, sem, *, levels):
    ny, nx, nz, _ = run.shape
    half = ny // 2
    odd = s[ODD_Z]
    scale = 1.0 / levels
    copies = []
    for y in range(half):
        for ref, base in ((own, odd * half), (got, (1 - odd) * half)):
            row = base + y

            def body(x, _, ref=ref, row=row, y=y):
                low = jnp.broadcast_to(ref[pl.ds(y * nx + x, 1), :], (nz, 128))
                run[row, x] = (run[row, x] + low) * scale
                return 0

            lax.fori_loop(0, nx, body, 0, unroll=8)
            copies.append(
                pltpu.make_async_copy(run.at[row], out.at[row], sem.at[len(copies)])
            )
            copies[-1].start()
    for c in copies:
        c.wait()


def below(s, mine, other):
    n = lax.axis_size("pz")
    rows, nm = mine.shape
    whole, half = VMEM((rows, nm), jnp.float32), VMEM((rows // 2, nm), jnp.float32)
    r = lax.ppermute(other, "pz", flip(n, 1))
    mine2, other2 = call(halve_kernel, (half, half), (s, mine, r))
    r2 = lax.ppermute(other2, "pz", flip(n, 2))
    tot = call(add_kernel, half, (s, mine2, r2))
    q = lax.ppermute(tot, "pz", flip(n, 4))
    q2 = lax.ppermute(call(add_kernel, half, (s, tot, q)), "pz", flip(n, 8))
    sent, kept = call(back_kernel, (half, half), (s, mine2, r2, q, q2))
    got = lax.ppermute(sent, "pz", flip(n, 2))
    sent, kept = call(core_kernel, (whole, whole), (s, mine, r, kept, got))
    return kept, lax.ppermute(sent, "pz", flip(n, 1))


def swap(a, b, name):
    n = lax.axis_size(name)
    return lax.ppermute(a, name, pairs(n, 0)), lax.ppermute(b, name, pairs(n, 1))


def local(tracer, flow_y, flow_x, flow_z):
    ny, nx, nz, nm = tracer.shape
    s = table()
    f32 = jnp.float32
    block, whole = VMEM(tracer.shape, f32), jax.ShapeDtypeStruct(tracer.shape, f32)
    y_face = VMEM((nx, nz, nm), f32)
    z_face = VMEM((ny, nx, nm), f32)
    x_face = VMEM((ny, nz, nm), f32)
    half = VMEM((ny * nx // 2, nm), f32)

    ya, yb = call(
        first_kernel, (y_face, y_face), (s, (tracer,)), scratch=[pltpu.SemaphoreType.DMA((2,))]
    )
    t = tracer
    for step in range(STEPS):
        ya, yb = swap(ya, yb, "py")
        za, zb, xa, xb = call(face_kernel, (z_face, z_face, x_face, x_face), (s, t))
        za, zb = swap(za, zb, "pz")
        xa, xb = swap(xa, xb, "px")
        u = call(
            main_kernel, block, (s, t, flow_y, flow_x, flow_z, za, zb, xa, xb),
            flops=30_000_000,
            scratch=[pltpu.VMEM((ny * nx, nm), f32)] * 2,
        )
        if step < STEPS - 1:
            t, ya, yb = call(
                fix_kernel, (block, y_face, y_face), (s, u, flow_y, ya, yb), aliases={1: 0}
            )
    _, t, run, mine, other = call(
        last_kernel, (block, whole, block, half, half), (s, u, flow_y, ya, yb),
        aliases={1: 0}, scratch=[pltpu.SemaphoreType.DMA((ny,))],
    )
    kept, got = below(s, mine, other)
    levels = nz * lax.axis_size("pz")
    potential = call(
        functools.partial(end_kernel, levels=levels), whole, (s, run, kept, got),
        scratch=[pltpu.SemaphoreType.DMA((ny,))],
    )
    return potential, t


def solution(mesh):
    spec = P("py", "px", "pz", None)
    return jax.shard_map(
        local, mesh=mesh, in_specs=(spec,) * 4, out_specs=(spec,) * 2, check_vma=False
    )
```

```python
import functools

import jax
import jax.numpy as jnp
from jax import lax
from jax.experimental import pallas as pl
from jax.experimental.pallas import tpu as pltpu
from jax.sharding import PartitionSpec as P


STEPS = 4
PARTS = 2
LOADS = 3
RUNS = 2
RATE = 0.05
VMEM = pltpu.VMEM
LIMIT = 8 * 1024 * 1024


def pairs(n, k):
    perm = []
    for i in range(k, n, 2):
        j = (i + 1) % n
        perm += [(i, j), (j, i)]
    return perm


def flip(n, bit):
    return [(i, i ^ bit) for i in range(n)]


def across(n):
    chips = n // 2
    perm = []
    for i in range(n):
        chip, core = i // 2, i % 2
        other = chips - 2 - chip if chip % 2 == 0 else chips - chip
        perm.append((i, 2 * (other % chips) + core))
    return perm


def call(body, outs, args, flops=1_000_000, aliases=None, scratch=()):
    in_specs, operands = [], []
    for a in args:
        space = pltpu.HBM if isinstance(a, tuple) else VMEM
        in_specs.append(pl.BlockSpec(memory_space=space))
        operands.append(
            pltpu.with_memory_space_constraint(a[0] if isinstance(a, tuple) else a, space)
        )
    outs = outs if isinstance(outs, tuple) else (outs,)
    out_specs = [
        pl.BlockSpec(memory_space=pltpu.HBM if isinstance(o, jax.ShapeDtypeStruct) else VMEM)
        for o in outs
    ]
    result = pl.pallas_call(
        body,
        out_shape=outs,
        in_specs=in_specs,
        out_specs=tuple(out_specs),
        scratch_shapes=scratch,
        input_output_aliases=aliases or {},
        compiler_params=pltpu.CompilerParams(vmem_limit_bytes=LIMIT),
        cost_estimate=pl.CostEstimate(flops=flops, bytes_accessed=1024, transcendentals=0),
    )(*operands)
    return result if len(outs) > 1 else result[0]


def where_at(name):
    i, n = lax.axis_index(name), lax.axis_size(name)
    inside = jnp.where((i == 0) | (i == n - 1), 0.0, 1.0)
    return lax.rem(i, 2), inside.astype(jnp.float32)


def bit_of(k):
    return lax.rem(lax.div(lax.axis_index("pz"), k), 2)


def y_faces(t, ya, yb):
    ny, nx, _, _ = t.shape
    odd, keep = where_at("py")
    odd = odd == 1

    def rows(i, _):
        lo, hi = t[0, i], t[ny - 1, i]
        ya[i] = jnp.where(odd, lo, hi)
        yb[i] = jnp.where(odd, hi, lo) * keep
        return 0

    lax.fori_loop(0, nx, rows, 0, unroll=8)


def first_kernel(t, ya, yb, sem):
    ny = t.shape[0]
    odd, keep = where_at("py")
    copies = [
        pltpu.make_async_copy(t.at[(ny - 1) * (1 - odd)], ya, sem.at[0]),
        pltpu.make_async_copy(t.at[(ny - 1) * odd], yb, sem.at[1]),
    ]
    for c in copies:
        c.start()
    for c in copies:
        c.wait()

    def rows(i, _):
        yb[i] = yb[i] * keep
        return 0

    lax.fori_loop(0, ya.shape[0], rows, 0, unroll=8)


def face_kernel(t, started, za, zb, xa, xb):
    del started
    ny, nx, nz, _ = t.shape
    odd_z, keep_z = where_at("pz")
    odd_z = odd_z == 1
    flat = t.reshape(ny * nx * nz, 128)
    za_f, zb_f = za.reshape(ny * nx, 128), zb.reshape(ny * nx, 128)

    def cols(i, _):
        base = pl.multiple_of(i * 8 * nz, 8 * nz)
        lo = flat[pl.ds(base, 8, stride=nz), :]
        hi = flat[pl.ds(base + nz - 1, 8, stride=nz), :]
        at = pl.ds(pl.multiple_of(i * 8, 8), 8)
        za_f[at, :] = jnp.where(odd_z, lo, hi)
        zb_f[at, :] = jnp.where(odd_z, hi, lo) * keep_z
        return 0

    lax.fori_loop(0, ny * nx // 8, cols, 0, unroll=8)
    odd_x, keep_x = where_at("px")
    odd_x = odd_x == 1
    for y in range(ny):
        lo, hi = t[y, 0], t[y, nx - 1]
        xa[y] = jnp.where(odd_x, lo, hi)
        xb[y] = jnp.where(odd_x, hi, lo) * keep_x


def main_kernel(t, fy, fx, fz, out, ready=lambda y: None):
    ny, nx, nz, _ = t.shape
    iota = lax.broadcasted_iota(jnp.int32, (nz, 128), 0)
    is_lo, is_hi = iota == 0, iota == nz - 1
    zero = jnp.zeros((nz, 128), jnp.float32)

    def cell(y, x, back, mid, ahead, down_y, up_y):
        down_z = jnp.where(is_lo, 0.0, pltpu.roll(mid, 1, axis=0))
        up_z = jnp.where(is_hi, 0.0, pltpu.roll(mid, nz - 1, axis=0))
        spread = (down_z + up_z) + (back + ahead)
        slope = fx[y, x] * (ahead - back) + fz[y, x] * (up_z - down_z)
        if down_y is None:
            slope = slope + fy[y, x] * up_y
            spread = spread + up_y
        elif up_y is None:
            slope = slope - fy[y, x] * down_y
            spread = spread + down_y
        else:
            slope = slope + fy[y, x] * (up_y - down_y)
            spread = spread + (up_y + down_y)
        out[y, x] = (1.0 - 6.0 * RATE) * mid - slope + RATE * spread

    def line(y, first, last):
        def step(x, back, mid, ahead):
            cell(
                y, x, back, mid, ahead,
                None if first else t[y - 1, x],
                None if last else t[y + 1, x],
            )

        def body(x, carry):
            back, mid = carry
            ahead = t[y, x + 1]
            step(x, back, mid, ahead)
            return mid, ahead

        back, mid = lax.fori_loop(0, nx - 1, body, (zero, t[y, 0]), unroll=5)
        step(nx - 1, back, mid, zero)

    ready(0)
    line(0, True, False)

    def inner(y, _):
        ready(y)
        line(y, False, False)
        return 0

    lax.fori_loop(1, ny - 1, inner, 0)
    ready(ny - 1)
    line(ny - 1, False, True)


def load_main_kernel(*refs):
    t, *flows = refs[:4]
    count = sum(f.shape == t.shape for f in refs[5:-1])
    kept, out, sem = refs[5:-1], refs[4], refs[-1]
    ny = t.shape[0]
    near = list(flows)
    near[:count] = kept

    def copy(k, y):
        return pltpu.make_async_copy(flows[k].at[y], kept[k].at[y], sem.at[k, y])

    for y in range(ny):
        for k in range(count):
            copy(k, y).start()

    def ready(y):
        for k in range(count):
            copy(k, y).wait()

    main_kernel(t, *near, out, ready=ready)


def around_kernel(u_in, fz, fx, za, zb, xa, xb, u):
    del u_in
    ny, nx, nz, _ = u.shape
    odd, _ = where_at("pz")
    odd = odd == 1
    flat, flow = u.reshape(ny * nx * nz, 128), fz.reshape(ny * nx * nz, 128)
    za_f, zb_f = za.reshape(ny * nx, 128), zb.reshape(ny * nx, 128)

    def cols(i, _):
        base = pl.multiple_of(i * 8 * nz, 8 * nz)
        at = pl.ds(pl.multiple_of(i * 8, 8), 8)
        a, b = za_f[at, :], zb_f[at, :]
        lo, hi = pl.ds(base, 8, stride=nz), pl.ds(base + nz - 1, 8, stride=nz)
        flat[lo, :] = flat[lo, :] + (RATE + flow[lo, :]) * jnp.where(odd, a, b)
        flat[hi, :] = flat[hi, :] + (RATE - flow[hi, :]) * jnp.where(odd, b, a)
        return 0

    lax.fori_loop(0, ny * nx // 8, cols, 0, unroll=8)
    odd_x, _ = where_at("px")
    odd_x = odd_x == 1
    for y in range(ny):
        a, b = xa[y], xb[y]
        u[y, 0] = u[y, 0] + (RATE + fx[y, 0]) * jnp.where(odd_x, a, b)
        u[y, nx - 1] = u[y, nx - 1] + (RATE - fx[y, nx - 1]) * jnp.where(odd_x, b, a)


def fix_rows(u, fy, ya, yb):
    ny, nx, _, _ = u.shape
    odd, _ = where_at("py")
    odd = odd == 1

    def body(x, _):
        a, b = ya[x], yb[x]
        lo, hi = jnp.where(odd, a, b), jnp.where(odd, b, a)
        u[0, x] = u[0, x] + (RATE + fy[0, x]) * lo
        u[ny - 1, x] = u[ny - 1, x] + (RATE - fy[ny - 1, x]) * hi
        return 0

    lax.fori_loop(0, nx, body, 0, unroll=8)


def fix_kernel(u_in, fy, ya_in, yb_in, u, ya, yb):
    del u_in
    fix_rows(u, fy, ya_in, yb_in)
    y_faces(u, ya, yb)


def last_kernel(u_in, fy, ya_in, yb_in, u, *totals):
    del u_in
    ny, nx, nz, _ = u.shape
    fix_rows(u, fy, ya_in, yb_in)
    flat = u.reshape(ny * nx * nz, 128)
    half, count = ny * nx // 2, len(totals) // 2
    odd, _ = where_at("pz")
    for p in range(count):

        def cols(i, _, p=p):
            at = pl.ds(pl.multiple_of(i * 8, 8), 8)
            for bit, ref in ((1 - odd, totals[count + p]), (odd, totals[p])):
                base = (bit * half + p * (half // count) + i * 8) * nz
                base = pl.multiple_of(base, 8 * nz)
                parts = [flat[pl.ds(base + k, 8, stride=nz), :] for k in range(nz)]
                while len(parts) > 1:
                    parts = [a + b for a, b in zip(parts[::2], parts[1::2])]
                ref[at, :] = parts[0]
            return 0

        lax.fori_loop(0, half // count // 8, cols, 0, unroll=4)


def run_kernel(u, *refs, first, rows):
    out, run, sem = refs[-3:]
    _, nx, nz, _ = u.shape
    copies = [
        pltpu.make_async_copy(u.at[y], out.at[y], sem.at[y - first])
        for y in range(first, first + rows)
    ]
    for c in copies:
        c.start()
    iota = lax.broadcasted_iota(jnp.int32, (nz, 128), 0)
    keep = [iota >= d for d in (1, 2, 4)]

    def line(y, _):
        def body(x, _):
            v = u[y, x]
            for d, m in zip((1, 2, 4), keep):
                v = v + jnp.where(m, pltpu.roll(v, d, axis=0), 0.0)
            run[y, x] = v
            return 0

        return lax.fori_loop(0, nx, body, 0, unroll=8)

    lax.fori_loop(first, first + rows, line, 0)
    for c in copies:
        c.wait()


def over_rows(ref, body, unroll=4):
    def step(i, _):
        body(pl.ds(pl.multiple_of(i * 8, 8), 8))
        return 0

    lax.fori_loop(0, ref.shape[0] // 8, step, 0, unroll=unroll)


def halve_kernel(mine, r, mine2, other2):
    half = mine2.shape[0]
    bit = bit_of(2)

    def body(at):
        for b, ref in ((bit, mine2), (1 - bit, other2)):
            src = pl.ds(pl.multiple_of(b * half + at.start, 8), 8)
            ref[at, :] = mine[src, :] + r[src, :]

    over_rows(mine2, body)


def add_kernel(a, b, out):
    def body(at):
        out[at, :] = a[at, :] + b[at, :]

    over_rows(out, body)


def back_kernel(mine2, r2, q, q2, sent, kept):
    b1, b2, b3 = (bit_of(k).astype(jnp.float32) for k in (2, 4, 8))

    def body(at):
        pre = b2 * q[at, :] + b3 * q2[at, :]
        sent[at, :] = pre + (1.0 - b1) * mine2[at, :]
        kept[at, :] = pre + b1 * r2[at, :]

    over_rows(sent, body)


def core_kernel(mine, r, kept1, got1, sent, kept):
    half = kept1.shape[0]
    odd = bit_of(1).astype(jnp.float32)
    bit = bit_of(2)

    def body(at):
        for b, ref in ((bit, kept1), (1 - bit, got1)):
            dst = pl.ds(pl.multiple_of(b * half + at.start, 8), 8)
            pre = ref[at, :]
            sent[dst, :] = pre + (1.0 - odd) * mine[dst, :]
            kept[dst, :] = pre + odd * r[dst, :]

    over_rows(kept1, body)


def end_kernel(*refs, levels, partner, first):
    run, low, out, sem = refs[0], refs[1], refs[-2], refs[-1]
    ny, nx, nz, _ = run.shape
    rows = low.shape[0] // nx
    odd, _ = where_at("pz")
    base = ((1 - odd) if partner else odd) * (ny // 2) + first
    scale = 1.0 / levels
    copies = []
    for y in range(rows):
        row = base + y

        def body(x, _, row=row, y=y):
            under = jnp.broadcast_to(low[pl.ds(y * nx + x, 1), :], (nz, 128))
            run[row, x] = (run[row, x] + under) * scale
            return 0

        lax.fori_loop(0, nx, body, 0, unroll=8)
        copies.append(pltpu.make_async_copy(run.at[row], out.at[row], sem.at[y]))
        copies[-1].start()
    for c in copies:
        c.wait()


def below(mine, other):
    n = lax.axis_size("pz")
    rows, nm = mine.shape
    whole, half = VMEM((rows, nm), jnp.float32), VMEM((rows // 2, nm), jnp.float32)
    r = lax.ppermute(other, "pz", flip(n, 1))
    mine2, other2 = call(halve_kernel, (half, half), (mine, r))
    r2 = lax.ppermute(other2, "pz", flip(n, 2))
    tot = call(add_kernel, half, (mine2, r2))
    q = lax.ppermute(tot, "pz", flip(n, 4))
    tot = call(add_kernel, half, (tot, q))
    q2 = lax.ppermute(tot, "pz", across(n))
    sent, kept = call(back_kernel, (half, half), (mine2, r2, q, q2))
    got = lax.ppermute(sent, "pz", flip(n, 2))
    sent, kept = call(core_kernel, (whole, whole), (mine, r, kept, got))
    return kept, lax.ppermute(sent, "pz", flip(n, 1))


def swap(a, b, name):
    n = lax.axis_size(name)
    a = lax.ppermute(a, name, pairs(n, 0))
    b = lax.ppermute(b, name, pairs(n, 1))
    return a, b


def local(tracer, flow_y, flow_x, flow_z):
    ny, nx, nz, nm = tracer.shape
    f32 = jnp.float32
    block, whole = VMEM(tracer.shape, f32), jax.ShapeDtypeStruct(tracer.shape, f32)
    y_face = VMEM((nx, nz, nm), f32)
    z_face = VMEM((ny, nx, nm), f32)
    x_face = VMEM((ny, nz, nm), f32)
    dma = pltpu.SemaphoreType.DMA

    ya, yb = call(first_kernel, (y_face, y_face), ((tracer,),), 60_000_000, scratch=[dma((2,))])
    t, started = tracer, ya
    flows = [flow_y, flow_x, flow_z]
    for step in range(STEPS):
        ya, yb = swap(ya, yb, "py")
        za, zb, xa, xb = call(
            face_kernel, (z_face, z_face, x_face, x_face), (t, started),
            60_000_000 if step == 0 else 1_000_000,
        )
        za, zb = swap(za, zb, "pz")
        xa, xb = swap(xa, xb, "px")
        if step == 0:
            u, *kept = call(
                load_main_kernel, (block,) * (1 + LOADS),
                (t, *((f,) for f in flows[:LOADS]), *flows[LOADS:]),
                flops=30_000_000, scratch=[dma((LOADS, ny))],
            )
            flows[:LOADS] = kept
        else:
            u = call(main_kernel, block, (t, *flows), flops=30_000_000)
        flow_y, flow_x, flow_z = flows
        u = call(around_kernel, block, (u, flow_z, flow_x, za, zb, xa, xb), aliases={0: 0})
        if step < STEPS - 1:
            t, ya, yb = call(
                fix_kernel, (block, y_face, y_face), (u, flow_y, ya, yb), aliases={0: 0}
            )
            started = ya
    part = VMEM((ny * nx // 2 // PARTS, nm), f32)
    t, *totals = call(
        last_kernel, (block,) + (part,) * (2 * PARTS), (u, flow_y, ya, yb), aliases={0: 0}
    )
    levels = nz * lax.axis_size("pz")
    rows = ny // 2 // PARTS
    field, state = t, ()
    for k in range(RUNS):
        body = functools.partial(run_kernel, first=k * (ny // RUNS), rows=ny // RUNS)
        state = call(
            body, (whole, block), (field, *state), flops=6_000_000,
            aliases={1: 0, 2: 1} if state else None, scratch=[dma((ny // RUNS,))],
        )
        state = ((state[0],), state[1])
    (t,), run = state
    lows = []
    for p in range(PARTS):
        lows.append(below(totals[p], totals[PARTS + p]))
    potential = None
    for p, pair in enumerate(lows):
        for partner, low in enumerate(pair):
            body = functools.partial(
                end_kernel, levels=levels, partner=bool(partner), first=p * rows
            )
            done = () if potential is None else ((potential,),)
            potential = call(
                body, whole, (run, low) + done, aliases={2: 0} if done else None,
                scratch=[dma((rows,))],
            )
    return potential, t


def solution(mesh):
    spec = P("py", "px", "pz", None)
    return jax.shard_map(
        local, mesh=mesh, in_specs=(spec,) * 4, out_specs=(spec,) * 2, check_vma=False
    )
```

```python
import functools

import jax
import jax.numpy as jnp
from jax import lax
from jax.experimental import pallas as pl
from jax.experimental.pallas import tpu as pltpu
from jax.sharding import PartitionSpec as P


STEPS = 4
LOADS = 3
RUNS = 2
ENDS = (((0, 0),), ((0, 1), (1, 0)), ((1, 1),))
RATE = 0.05
VMEM = pltpu.VMEM
LIMIT = 8 * 1024 * 1024


def pairs(n, k):
    perm = []
    for i in range(k, n, 2):
        j = (i + 1) % n
        perm += [(i, j), (j, i)]
    return perm


def flip(n, bit):
    return [(i, i ^ bit) for i in range(n)]


def across(n):
    chips = n // 2
    perm = []
    for i in range(n):
        chip, core = i // 2, i % 2
        other = chips - 2 - chip if chip % 2 == 0 else chips - chip
        perm.append((i, 2 * (other % chips) + core))
    return perm


def call(body, outs, args, flops=1_000_000, aliases=None, scratch=()):
    in_specs, operands = [], []
    for a in args:
        space = pltpu.HBM if isinstance(a, tuple) else VMEM
        in_specs.append(pl.BlockSpec(memory_space=space))
        operands.append(
            pltpu.with_memory_space_constraint(a[0] if isinstance(a, tuple) else a, space)
        )
    outs = outs if isinstance(outs, tuple) else (outs,)
    out_specs = [
        pl.BlockSpec(memory_space=pltpu.HBM if isinstance(o, jax.ShapeDtypeStruct) else VMEM)
        for o in outs
    ]
    result = pl.pallas_call(
        body,
        out_shape=outs,
        in_specs=in_specs,
        out_specs=tuple(out_specs),
        scratch_shapes=scratch,
        input_output_aliases=aliases or {},
        compiler_params=pltpu.CompilerParams(vmem_limit_bytes=LIMIT),
        cost_estimate=pl.CostEstimate(flops=flops, bytes_accessed=1024, transcendentals=0),
    )(*operands)
    return result if len(outs) > 1 else result[0]


def where_at(name):
    i, n = lax.axis_index(name), lax.axis_size(name)
    inside = jnp.where((i == 0) | (i == n - 1), 0.0, 1.0)
    return lax.rem(i, 2), inside.astype(jnp.float32)


def bit_of(k):
    return lax.rem(lax.div(lax.axis_index("pz"), k), 2)


def first_kernel(t, ya, yb, sem):
    ny, nx, _, _ = t.shape
    odd, keep = where_at("py")
    chunks = sem.shape[1]
    size = nx // chunks
    copies = []
    for k in range(chunks):
        at = pl.ds(k * size, size)
        for j, (row, ref) in enumerate((((ny - 1) * (1 - odd), ya), ((ny - 1) * odd, yb))):
            copies.append(pltpu.make_async_copy(t.at[row, at], ref.at[at], sem.at[j, k]))
            copies[-1].start()
    for c in copies:
        c.wait()

    @pl.when(keep == 0.0)
    def _():
        def rows(i, _):
            yb[i] = jnp.zeros_like(yb[i])
            return 0

        lax.fori_loop(0, nx, rows, 0, unroll=8)


def face_kernel(t, started, za, zb, xa, xb):
    del started
    ny, nx, nz, _ = t.shape
    odd_z, keep_z = where_at("pz")
    odd_z = odd_z == 1
    flat = t.reshape(ny * nx * nz, 128)
    za_f, zb_f = za.reshape(ny * nx, 128), zb.reshape(ny * nx, 128)

    def cols(i, _):
        base = pl.multiple_of(i * 8 * nz, 8 * nz)
        lo = flat[pl.ds(base, 8, stride=nz), :]
        hi = flat[pl.ds(base + nz - 1, 8, stride=nz), :]
        at = pl.ds(pl.multiple_of(i * 8, 8), 8)
        za_f[at, :] = jnp.where(odd_z, lo, hi)
        zb_f[at, :] = jnp.where(odd_z, hi, lo) * keep_z
        return 0

    lax.fori_loop(0, ny * nx // 8, cols, 0, unroll=8)
    odd_x, keep_x = where_at("px")
    odd_x = odd_x == 1
    for y in range(ny):
        lo, hi = t[y, 0], t[y, nx - 1]
        xa[y] = jnp.where(odd_x, lo, hi)
        xb[y] = jnp.where(odd_x, hi, lo) * keep_x


def main_kernel(t, fy, fx, fz, out, ready=lambda y: None):
    ny, nx, nz, _ = t.shape
    iota = lax.broadcasted_iota(jnp.int32, (nz, 128), 0)
    is_lo, is_hi = iota == 0, iota == nz - 1
    zero = jnp.zeros((nz, 128), jnp.float32)

    def cell(y, x, back, mid, ahead, down_y, up_y):
        down_z = jnp.where(is_lo, 0.0, pltpu.roll(mid, 1, axis=0))
        up_z = jnp.where(is_hi, 0.0, pltpu.roll(mid, nz - 1, axis=0))
        spread = (down_z + up_z) + (back + ahead)
        slope = fx[y, x] * (ahead - back) + fz[y, x] * (up_z - down_z)
        if down_y is None:
            slope = slope + fy[y, x] * up_y
            spread = spread + up_y
        elif up_y is None:
            slope = slope - fy[y, x] * down_y
            spread = spread + down_y
        else:
            slope = slope + fy[y, x] * (up_y - down_y)
            spread = spread + (up_y + down_y)
        out[y, x] = (1.0 - 6.0 * RATE) * mid - slope + RATE * spread

    def line(y, first, last):
        def step(x, back, mid, ahead):
            cell(
                y, x, back, mid, ahead,
                None if first else t[y - 1, x],
                None if last else t[y + 1, x],
            )

        def body(x, carry):
            back, mid = carry
            ahead = t[y, x + 1]
            step(x, back, mid, ahead)
            return mid, ahead

        back, mid = lax.fori_loop(0, nx - 1, body, (zero, t[y, 0]), unroll=5)
        step(nx - 1, back, mid, zero)

    ready(0)
    line(0, True, False)

    def inner(y, _):
        ready(y)
        line(y, False, False)
        return 0

    lax.fori_loop(1, ny - 1, inner, 0)
    ready(ny - 1)
    line(ny - 1, False, True)


def load_main_kernel(*refs):
    t, *flows = refs[:4]
    count = sum(f.shape == t.shape for f in refs[5:-1])
    kept, out, sem = refs[5:-1], refs[4], refs[-1]
    ny = t.shape[0]
    near = list(flows)
    near[:count] = kept

    def copy(k, y):
        return pltpu.make_async_copy(flows[k].at[y], kept[k].at[y], sem.at[k, y])

    for y in range(ny):
        for k in range(count):
            copy(k, y).start()

    def ready(y):
        for k in range(count):
            copy(k, y).wait()

    main_kernel(t, *near, out, ready=ready)


def around_kernel(u_in, fz, fx, za, zb, xa, xb, u):
    del u_in
    ny, nx, nz, _ = u.shape
    odd, _ = where_at("pz")
    odd = odd == 1
    flat, flow = u.reshape(ny * nx * nz, 128), fz.reshape(ny * nx * nz, 128)
    za_f, zb_f = za.reshape(ny * nx, 128), zb.reshape(ny * nx, 128)

    def cols(i, _):
        base = pl.multiple_of(i * 8 * nz, 8 * nz)
        at = pl.ds(pl.multiple_of(i * 8, 8), 8)
        a, b = za_f[at, :], zb_f[at, :]
        lo, hi = pl.ds(base, 8, stride=nz), pl.ds(base + nz - 1, 8, stride=nz)
        flat[lo, :] = flat[lo, :] + (RATE + flow[lo, :]) * jnp.where(odd, a, b)
        flat[hi, :] = flat[hi, :] + (RATE - flow[hi, :]) * jnp.where(odd, b, a)
        return 0

    lax.fori_loop(0, ny * nx // 8, cols, 0, unroll=8)
    odd_x, _ = where_at("px")
    odd_x = odd_x == 1
    for y in range(ny):
        a, b = xa[y], xb[y]
        u[y, 0] = u[y, 0] + (RATE + fx[y, 0]) * jnp.where(odd_x, a, b)
        u[y, nx - 1] = u[y, nx - 1] + (RATE - fx[y, nx - 1]) * jnp.where(odd_x, b, a)


def fix_rows(u, fy, ya, yb):
    ny, nx, _, _ = u.shape
    odd, _ = where_at("py")
    odd = odd == 1

    def body(x, _):
        a, b = ya[x], yb[x]
        lo, hi = jnp.where(odd, a, b), jnp.where(odd, b, a)
        u[0, x] = u[0, x] + (RATE + fy[0, x]) * lo
        u[ny - 1, x] = u[ny - 1, x] + (RATE - fy[ny - 1, x]) * hi
        return 0

    lax.fori_loop(0, nx, body, 0, unroll=8)


def fix_kernel(u_in, fy, ya_in, yb_in, u, ya, yb):
    del u_in
    ny, nx, _, _ = u.shape
    odd, keep = where_at("py")
    odd = odd == 1

    def body(x, _):
        a, b = ya_in[x], yb_in[x]
        lo, hi = jnp.where(odd, a, b), jnp.where(odd, b, a)
        lo = u[0, x] + (RATE + fy[0, x]) * lo
        hi = u[ny - 1, x] + (RATE - fy[ny - 1, x]) * hi
        u[0, x] = lo
        u[ny - 1, x] = hi
        ya[x] = jnp.where(odd, lo, hi)
        yb[x] = jnp.where(odd, hi, lo) * keep
        return 0

    lax.fori_loop(0, nx, body, 0, unroll=8)


def part_rows(part, bit, ny):
    inner = [1 + k + bit * (ny // 2) for k in range(ny // 2 - 2)]
    return [bit * (ny - 1), ny // 2 - 1 + bit] if part else inner


def block_totals(u, mine, other, part):
    ny, nx, nz, _ = u.shape
    flat = u.reshape(ny * nx * nz, 128)
    odd, _ = where_at("pz")
    for bit, ref in ((1 - odd, other), (odd, mine)):
        for k, row in enumerate(part_rows(part, bit, ny)):

            def cols(i, _, ref=ref, row=row, k=k):
                base = pl.multiple_of((row * nx + i * 8) * nz, 8 * nz)
                parts = [flat[pl.ds(base + z, 8, stride=nz), :] for z in range(nz)]
                while len(parts) > 1:
                    parts = [a + b for a, b in zip(parts[::2], parts[1::2])]
                ref[pl.ds(pl.multiple_of(k * nx + i * 8, 8), 8), :] = parts[0]
                return 0

            lax.fori_loop(0, nx // 8, cols, 0, unroll=4)


def inner_kernel(u_in, u, mine, other):
    del u_in
    block_totals(u, mine, other, 0)


def last_kernel(u_in, fy, ya_in, yb_in, u, mine, other):
    del u_in
    fix_rows(u, fy, ya_in, yb_in)
    block_totals(u, mine, other, 1)


def run_kernel(u, *refs, first, rows):
    out, run, sem = refs[-3:]
    _, nx, nz, _ = u.shape
    copies = [
        pltpu.make_async_copy(u.at[y], out.at[y], sem.at[y - first])
        for y in range(first, first + rows)
    ]
    for c in copies:
        c.start()
    iota = lax.broadcasted_iota(jnp.int32, (nz, 128), 0)
    keep = [iota >= d for d in (1, 2, 4)]

    def line(y, _):
        def body(x, _):
            v = u[y, x]
            for d, m in zip((1, 2, 4), keep):
                v = v + jnp.where(m, pltpu.roll(v, d, axis=0), 0.0)
            run[y, x] = v
            return 0

        return lax.fori_loop(0, nx, body, 0, unroll=8)

    lax.fori_loop(first, first + rows, line, 0)
    for c in copies:
        c.wait()


def over_rows(ref, body, unroll=6):
    def step(i, _):
        body(pl.ds(pl.multiple_of(i * 8, 8), 8))
        return 0

    lax.fori_loop(0, ref.shape[0] // 8, step, 0, unroll=unroll)


def halve_kernel(mine, r, mine2, other2):
    half = mine2.shape[0]
    bit = bit_of(2)

    def body(at):
        for b, ref in ((bit, mine2), (1 - bit, other2)):
            src = pl.ds(pl.multiple_of(b * half + at.start, 8), 8)
            ref[at, :] = mine[src, :] + r[src, :]

    over_rows(mine2, body)


def add_kernel(a, b, out):
    def body(at):
        out[at, :] = a[at, :] + b[at, :]

    over_rows(out, body)


def back_kernel(mine2, r2, q, q2, sent, kept):
    b1, b2, b3 = (bit_of(k).astype(jnp.float32) for k in (2, 4, 8))

    def body(at):
        pre = b2 * q[at, :] + b3 * q2[at, :]
        sent[at, :] = pre + (1.0 - b1) * mine2[at, :]
        kept[at, :] = pre + b1 * r2[at, :]

    over_rows(sent, body)


def core_kernel(mine, r, kept1, got1, sent, kept):
    half = kept1.shape[0]
    odd = bit_of(1).astype(jnp.float32)
    bit = bit_of(2)

    def body(at):
        for b, ref in ((bit, kept1), (1 - bit, got1)):
            dst = pl.ds(pl.multiple_of(b * half + at.start, 8), 8)
            pre = ref[at, :]
            sent[dst, :] = pre + (1.0 - odd) * mine[dst, :]
            kept[dst, :] = pre + odd * r[dst, :]

    over_rows(kept1, body)


def end_kernel(run, *refs, levels, pieces):
    out, sem = refs[-2:]
    ny, nx, nz, _ = run.shape
    odd, _ = where_at("pz")
    scale = 1.0 / levels
    copies = []
    for low, (part, partner) in zip(refs, pieces):
        for y, row in enumerate(part_rows(part, (1 - odd) if partner else odd, ny)):

            def body(x, _, low=low, row=row, y=y):
                under = jnp.broadcast_to(low[pl.ds(y * nx + x, 1), :], (nz, 128))
                run[row, x] = (run[row, x] + under) * scale
                return 0

            lax.fori_loop(0, nx, body, 0, unroll=8)
            copies.append(
                pltpu.make_async_copy(run.at[row], out.at[row], sem.at[len(copies)])
            )
            copies[-1].start()
    for c in copies:
        c.wait()


def below(mine, other):
    n = lax.axis_size("pz")
    rows, nm = mine.shape
    whole, half = VMEM((rows, nm), jnp.float32), VMEM((rows // 2, nm), jnp.float32)
    r = lax.ppermute(other, "pz", flip(n, 1))
    mine2, other2 = call(halve_kernel, (half, half), (mine, r))
    r2 = lax.ppermute(other2, "pz", flip(n, 2))
    tot = call(add_kernel, half, (mine2, r2))
    q = lax.ppermute(tot, "pz", flip(n, 4))
    tot = call(add_kernel, half, (tot, q))
    q2 = lax.ppermute(tot, "pz", across(n))
    sent, kept = call(back_kernel, (half, half), (mine2, r2, q, q2))
    got = lax.ppermute(sent, "pz", flip(n, 2))
    sent, kept = call(core_kernel, (whole, whole), (mine, r, kept, got))
    return kept, lax.ppermute(sent, "pz", flip(n, 1))


def swap(a, b, name):
    n = lax.axis_size(name)
    a = lax.ppermute(a, name, pairs(n, 0))
    b = lax.ppermute(b, name, pairs(n, 1))
    return a, b


def local(tracer, flow_y, flow_x, flow_z):
    ny, nx, nz, nm = tracer.shape
    f32 = jnp.float32
    block, whole = VMEM(tracer.shape, f32), jax.ShapeDtypeStruct(tracer.shape, f32)
    y_face = VMEM((nx, nz, nm), f32)
    z_face = VMEM((ny, nx, nm), f32)
    x_face = VMEM((ny, nz, nm), f32)
    dma = pltpu.SemaphoreType.DMA

    ya, yb = call(first_kernel, (y_face, y_face), ((tracer,),), 60_000_000, scratch=[dma((2, 1))])
    t, started = tracer, ya
    flows = [flow_y, flow_x, flow_z]
    for step in range(STEPS):
        ya, yb = swap(ya, yb, "py")
        za, zb, xa, xb = call(
            face_kernel, (z_face, z_face, x_face, x_face), (t, started),
            60_000_000 if step == 0 else 1_000_000,
        )
        za, zb = swap(za, zb, "pz")
        xa, xb = swap(xa, xb, "px")
        if step == 0:
            u, *kept = call(
                load_main_kernel, (block,) * (1 + LOADS),
                (t, *((f,) for f in flows[:LOADS]), *flows[LOADS:]),
                flops=30_000_000, scratch=[dma((LOADS, ny))],
            )
            flows[:LOADS] = kept
        else:
            u = call(main_kernel, block, (t, *flows), flops=30_000_000)
        flow_y, flow_x, flow_z = flows
        u = call(around_kernel, block, (u, flow_z, flow_x, za, zb, xa, xb), aliases={0: 0})
        if step < STEPS - 1:
            t, ya, yb = call(
                fix_kernel, (block, y_face, y_face), (u, flow_y, ya, yb), aliases={0: 0}
            )
            started = ya
    inner, outer = VMEM(((ny // 2 - 2) * nx, nm), f32), VMEM((2 * nx, nm), f32)
    levels = nz * lax.axis_size("pz")
    u, *totals = call(inner_kernel, (block, inner, inner), (u,), aliases={0: 0})
    lows = [below(*totals)]
    t, *totals = call(last_kernel, (block, outer, outer), (u, flow_y, ya, yb), aliases={0: 0})
    lows.append(below(*totals))
    field, state = t, ()
    for k in range(RUNS):
        body = functools.partial(run_kernel, first=k * (ny // RUNS), rows=ny // RUNS)
        state = call(
            body, (whole, block), (field, *state), flops=6_000_000,
            aliases={1: 0, 2: 1} if state else None, scratch=[dma((ny // RUNS,))],
        )
        state = ((state[0],), state[1])
    (t,), run = state
    potential = ()
    for pieces in ENDS:
        body = functools.partial(end_kernel, levels=levels, pieces=pieces)
        args = [run] + [lows[part][partner] for part, partner in pieces]
        potential = call(
            body, whole, (*args, *potential),
            aliases={len(args): 0} if potential else None, scratch=[dma((ny,))],
        )
        potential = ((potential,),)
    ((potential,),) = potential
    return potential, t


def solution(mesh):
    spec = P("py", "px", "pz", None)
    return jax.shard_map(
        local, mesh=mesh, in_specs=(spec,) * 4, out_specs=(spec,) * 2, check_vma=False
    )
```
